128 devices in a mesh: grp: 8 (over y_hi, z), pair: 16 (over x, y_lo, core).
Axes of the slice: x: 4, y: 4 (y_hi: 2, y_lo: 2; y = y_hi * 2 + y_lo), z: 4, core: 2. Of those that a mesh axis runs over, the one named last changes fastest.
Arguments:
- amplitudes: bfloat16 [128, 512, 512], P('pair', 'grp'), may hold values from -6 to 6
- cholesky: bfloat16 [512, 512, 2048], P('pair', 'grp'), may hold values from -0.09375 to 0.09375
Outputs:
- ladder_term: float32 [512, 4, 128], P('pair', None, 'grp')
The draws below stay inside these ranges and needn't reach their ends.
All inputs are finite; a program needn't handle non-finite values.
Results may differ from the reference program's by a relative error of at most 0.003.
Values may be sent and summed in bfloat16 or wider, within the bound.
No kernel may reach another device: no remote copies, remote signals or barrier semaphores. Data moves between devices by JAX's collectives and lax.ppermute only.
A program may use at most 128 MiB of HBM per device.

```python
import jax
import jax.numpy as jnp
from jax import lax

VIRT = 512
NAUX = 2048
A_WIN = 4
NPAIR = 128


def levels(own_key, shape, shards, low, high):
    loudness = 1.0
    for axis_at, shards_of in shards:
        draws = jax.random.uniform(jax.random.fold_in(jax.random.fold_in(own_key, 6), axis_at), (shards_of,), jnp.float32, low / len(shards), high / len(shards))
        loudness = loudness * jnp.repeat(jnp.exp(draws), shape[axis_at] // shards_of).reshape((-1,) + (1,) * (len(shape) - 1 - axis_at))
    return loudness


def bell_draw(own_key, dims, spread, bound, split=(), kind=jnp.bfloat16):
    entries = jax.random.normal(own_key, dims, jnp.float32) * spread
    if len(split) > 0:
        entries = levels(own_key, dims, split, -0.22, 0.18) * entries
    return jnp.clip(entries, min=-bound, max=bound).astype(kind)


def setup_inputs(seed: int = 0) -> dict:
    splits = jax.random.split(jax.random.key(seed), 3)
    amplitudes = bell_draw(splits[0], (NPAIR, VIRT, VIRT), 1.0, 6.0, ((0, 16), (1, 8)))
    cholesky = bell_draw(splits[1], (VIRT, VIRT, NAUX), ((VIRT * VIRT * NAUX) ** -0.25), 0.09375, ((0, 16), (1, 8)))
    return {"amplitudes": amplitudes, "cholesky": cholesky}


def reference(amplitudes, cholesky):
    tiles_count = 8
    tile_width = VIRT // tiles_count
    window_chol = cholesky[:A_WIN]
    flat_chol = cholesky.reshape(VIRT * VIRT, NAUX)

    def one_tile(running, tile_index):
        offset = (tile_index * tile_width).astype(jnp.int32)
        portion = lax.dynamic_slice_in_dim(window_chol, offset, tile_width, 1)
        product = lax.dot_general(flat_chol, portion.reshape(A_WIN * tile_width, NAUX), (((1,), (1,)), ((), ())), preferred_element_type=jnp.float32)
        integrals = product.astype(jnp.bfloat16).reshape(VIRT, VIRT, A_WIN, tile_width)
        amp_slice = lax.dynamic_slice_in_dim(amplitudes, offset, tile_width, 2)
        contrib = lax.dot_general(integrals, amp_slice, (((1, 3), (1, 2)), ((), ())), preferred_element_type=jnp.float32)
        return running + contrib, None

    initial = jnp.zeros((VIRT, A_WIN, NPAIR), jnp.float32)
    result, unused = lax.scan(one_tile, initial, jnp.arange(tiles_count, dtype=jnp.int32))
    return result
```

```python
import functools

import jax
import jax.numpy as jnp
from jax import lax
from jax.experimental import pallas as pl
from jax.experimental.pallas import tpu as pltpu
from jax.sharding import PartitionSpec as P

A_WIN = 4
AXES = ("grp", "pair")
DT = 8


def linear(x, y, z, c):
    return ((y // 2) * 4 + z) * 16 + (x * 2 + y % 2) * 2 + c


def moved(value, where):
    pairs = []
    for x in range(4):
        for y in range(4):
            for z in range(4):
                for c in range(2):
                    to = where(x, y, z, c)
                    if to is not None:
                        pairs.append(
                            (linear(x, y, z, c), linear(to[0] % 4, to[1] % 4, to[2] % 4, to[3]))
                        )
    return lax.ppermute(value, AXES, pairs)


def position():
    g, p = lax.axis_index("grp"), lax.axis_index("pair")
    return p // 4, (g // 4) * 2 + (p // 2) % 2, g % 4, p % 2


def gathered_window(cholesky, x, y, z, k):
    at_root = lambda x, y, z, c: x == 0 and y % 2 == 0 and c == 0
    got = [
        moved(cholesky[dx], lambda x, y, z, c: (dx, y, z, y // 2) if at_root(x, y, z, c) else None)
        for dx in (2, 1, 3)
    ]
    got.append(
        moved(cholesky[0], lambda x, y, z, c: (0, y, z, 1) if at_root(x, y, z, c) and y == 2 else None)
    )
    own = jnp.where((x == 0) & (y == 0) & (k == 0), cholesky[0], jnp.zeros_like(cholesky[0]))
    piece = own + got[0] + got[1] + got[2] + got[3]
    spread = [
        moved(piece, lambda x, y, z, c: (x, y + dy, z, c) if y == 2 * c else None) for dy in (2, 1, 3)
    ]
    piece = piece + spread[0] + spread[1] + spread[2]
    early = [piece] + [moved(piece, lambda x, y, z, c: (x, y, z - j, c)) for j in (1, 2, 3)]
    others = [moved(piece, lambda x, y, z, c: (x - dx, y, z, c)) for dx in (1, 2, 3)]
    others = jnp.stack(others)
    late = [others] + [moved(others, lambda x, y, z, c: (x, y, z - j, c)) for j in (1, 2, 3)]
    return early, late


def gathered_amplitudes(amplitudes, z, k):
    n_ij, n_d = amplitudes.shape[:2]
    parts = amplitudes.reshape(n_ij, n_d, 2, 4, 64).transpose(2, 3, 0, 1, 4).reshape(2, 4, n_ij, n_d * 64)
    twice = jnp.concatenate([parts, parts], axis=1)
    turned = lax.dynamic_slice_in_dim(twice, z, 4, 1)
    mine = lax.dynamic_index_in_dim(turned, k, 0, keepdims=False)
    other = lax.dynamic_index_in_dim(turned, 1 - k, 0, keepdims=False)
    came = moved(other, lambda x, y, z, c: (x, y, z, 1 - c))
    a0 = jnp.concatenate([mine, came], axis=1)
    across = lambda x, y, z, c: (x, y ^ 1, z, c)
    b0 = moved(a0, across)
    a = [a0] + [moved(a0, lambda x, y, z, c: (x - dx, y, z, c)) for dx in (1, 2, 3)]
    b1, b3 = [moved(b0, lambda x, y, z, c: (x - dx, y, z, c)) for dx in (1, 3)]
    b2 = moved(a[2], across)
    return [a[0], b0, a[1], b1, a[2], b2, a[3], b3]


NT = (((1,), (1,)), ((), ()))


def kernel(blocks, started, last, pos_ref, *refs):
    x_refs = refs[:2]
    w_refs = refs[2 : 2 + 2 * blocks]
    t_refs = refs[2 + 2 * blocks : 2 + 10 * blocks]
    rest = refs[2 + 10 * blocks :]
    acc_ref = rest[0] if started else None
    o_ref, wbuf, total = rest[-3:]
    step = pl.program_id(0)

    @pl.when(step == 0)
    def _():
        for n in range(blocks):
            wbuf[n, 0:64] = w_refs[2 * n][...]
            for r in range(3):
                wbuf[n, 64 * (r + 1) : 64 * (r + 2)] = w_refs[2 * n + 1][r]
        if started:
            total[...] = acc_ref[...]
        else:
            total[...] = jnp.zeros_like(total)

    for n in range(blocks):
        tile = []
        for h in range(2):
            rows = x_refs[h][...].reshape(DT * 32, -1)
            tile.append(
                lax.dot_general(rows, wbuf[n], NT, preferred_element_type=jnp.float32).astype(jnp.bfloat16)
            )
        amp = jnp.concatenate([t_refs[8 * n + r][0] for r in range(8)], axis=0)
        for q in range(DT // 4):
            left = []
            for h in range(2):
                for a in range(4):
                    left.append(
                        jnp.concatenate(
                            [
                                tile[h][(4 * q + d) * 32 : (4 * q + d + 1) * 32, a * 64 : (a + 1) * 64]
                                for d in range(4)
                            ],
                            axis=1,
                        )
                    )
            left = jnp.concatenate(left, axis=0)
            total[...] += lax.dot_general(
                amp[:, 256 * q : 256 * (q + 1)], left, NT, preferred_element_type=jnp.float32
            )

    @pl.when(step == pl.num_programs(0) - 1)
    def _():
        if last:
            x, low, k = pos_ref[0], pos_ref[1], pos_ref[2]
            for dx in range(4):
                for dy in range(2):
                    to = lax.rem(x + dx, 4) * 2 + (low + dy) % 2
                    for e in range(2):
                        row = (dx * 2 + dy) * 16 + e * 8
                        o_ref[to, (k + e) % 2] = total[row : row + 8, :]
        else:
            o_ref[...] = total[...]


def contracted(pos, chol, window, amps, js, acc, last):
    blocks = len(js)
    n_d = chol[0].shape[0]
    full = lambda shape: pl.BlockSpec(shape, lambda i, pos: (0,) * len(shape))
    in_specs = [pl.BlockSpec((DT, 32, 2048), lambda i, pos: (i, 0, 0))] * 2
    operands = list(chol)
    for j in js:
        in_specs += [full((64, 2048)), full((3, 64, 2048))]
        operands += [window[0][j], window[1][j]]
    for j in js:
        in_specs += [pl.BlockSpec((1, 16, DT * 64), lambda i, pos, j=j: (j, 0, i))] * 8
        operands += amps
    if acc is not None:
        in_specs.append(full((128, 256)))
        operands.append(acc)
    out = (8, 2, 8, 256) if last else (128, 256)
    return pl.pallas_call(
        functools.partial(kernel, blocks, acc is not None, last),
        grid_spec=pltpu.PrefetchScalarGridSpec(
            num_scalar_prefetch=1,
            grid=(n_d // DT,),
            in_specs=in_specs,
            out_specs=full(out),
            scratch_shapes=[
                pltpu.VMEM((blocks, 256, 2048), jnp.bfloat16),
                pltpu.VMEM((128, 256), jnp.float32),
            ],
        ),
        out_shape=jax.ShapeDtypeStruct(out, jnp.float32),
        compiler_params=pltpu.CompilerParams(vmem_limit_bytes=48 * 1024 * 1024),
        cost_estimate=pl.CostEstimate(
            flops=blocks * 2 * 4096 * 256 * 2048, bytes_accessed=20 * 1024 * 1024, transcendentals=0
        ),
    )(pos, *operands)


def per_device(amplitudes, cholesky):
    x, y, z, k = position()
    pos = jnp.stack([x, y % 2, k]).astype(jnp.int32)
    window = gathered_window(cholesky, x, y, z, k)
    amps = gathered_amplitudes(amplitudes, z, k)
    mine = cholesky.transpose(1, 0, 2)
    chol = (mine, moved(mine, lambda x, y, z, c: (x, y, z, 1 - c)))
    acc = contracted(pos, chol, window, amps, (0,), None, False)
    acc = contracted(pos, chol, window, amps, (1, 3), acc, False)
    parts = contracted(pos, chol, window, amps, (2,), acc, True).reshape(8, 16, 256)
    own = parts[:, :, :128] + moved(parts[:, :, 128:], lambda x, y, z, c: (x, y, z, 1 - c))
    blocks = lax.all_to_all(own, "grp", 0, 0, tiled=True)
    result = jnp.sum(blocks, axis=0).reshape(16, 4, 32)
    result = lax.dynamic_slice_in_dim(jnp.concatenate([result, result], axis=1), (4 - x) % 4, 4, 1)
    return result.transpose(2, 1, 0)


def solution(mesh):
    in_specs = (P("pair", "grp", None), P("pair", "grp", None))
    out_specs = P("pair", None, "grp")
    return jax.shard_map(
        per_device, mesh=mesh, in_specs=in_specs, out_specs=out_specs, check_vma=False
    )
```

```python
import functools

import jax
import jax.numpy as jnp
from jax import lax
from jax.experimental import pallas as pl
from jax.experimental.pallas import tpu as pltpu
from jax.sharding import PartitionSpec as P


AXES = ("grp", "pair")
DT = 16
VMEM_MIB = 48


def linear(x, y, z, c):
    return ((y // 2) * 4 + z) * 16 + (x * 2 + y % 2) * 2 + c


def moved(value, where):
    pairs = []
    for x in range(4):
        for y in range(4):
            for z in range(4):
                for c in range(2):
                    to = where(x, y, z, c)
                    if to is not None:
                        pairs.append(
                            (linear(x, y, z, c), linear(to[0] % 4, to[1] % 4, to[2] % 4, to[3]))
                        )
    return lax.ppermute(value, AXES, pairs)


def position():
    g, p = lax.axis_index("grp"), lax.axis_index("pair")
    return p // 4, (g // 4) * 2 + (p // 2) % 2, g % 4, p % 2


def gathered_window(cholesky, x, y, k):
    at_root = lambda x, y, c: x == 0 and y % 2 == 0 and c == 0
    got = [
        moved(cholesky[dx], lambda x, y, z, c: (dx, y, z, y // 2) if at_root(x, y, c) else None)
        for dx in (1, 3, 2)
    ]
    got.append(
        moved(cholesky[0], lambda x, y, z, c: (0, y, z, 1) if at_root(x, y, c) and y == 2 else None)
    )
    own = jnp.where((x == 0) & (y == 0) & (k == 0), cholesky[0], jnp.zeros_like(cholesky[0]))
    piece = own + got[0] + got[1] + got[2] + got[3]
    spread = [
        moved(piece, lambda x, y, z, c: (x, y + dy, z, c) if y == 2 * c else None)
        for dy in (1, 3, 2)
    ]
    piece = piece + spread[0] + spread[1] + spread[2]
    others = [moved(piece, lambda x, y, z, c: (x - dx, y, z, c)) for dx in (1, 3, 2)]
    early = [moved(piece, lambda x, y, z, c: (x, y, z - j, c)) for j in (1, 3, 2)]
    half = others[2].shape[0] // 2
    upper = jnp.concatenate([others[0], others[2][:half]])
    lower = jnp.concatenate([others[2][half:], others[1]])
    rise = lambda x, y, z, c: (x, y, z + 1, c)
    fall = lambda x, y, z, c: (x, y, z - 1, c)
    up, down = moved(upper, rise), moved(lower, fall)
    up_more, down_more = moved(lower, rise), moved(upper, fall)
    up_far, down_far = moved(up, rise), moved(down, fall)
    return [
        [piece, upper, lower],
        [early[0], down_more, down],
        [early[2], up_far, down_far],
        [early[1], up, up_more],
    ]


def gathered_amplitudes(amplitudes, z, k):
    n_ij, n_d = amplitudes.shape[:2]
    parts = amplitudes.reshape(n_ij, n_d, 2, 4, 64).transpose(2, 3, 0, 1, 4).reshape(2, 4, n_ij, n_d * 64)
    twice = jnp.concatenate([parts, parts], axis=1)
    turned = lax.dynamic_slice_in_dim(twice, z, 4, 1)
    mine = lax.dynamic_index_in_dim(turned, k, 0, keepdims=False)
    other = lax.dynamic_index_in_dim(turned, 1 - k, 0, keepdims=False)
    came = moved(other, lambda x, y, z, c: (x, y, z, 1 - c))
    a0 = jnp.concatenate([mine, came], axis=1)
    across = lambda x, y, z, c: (x, y ^ 1, z, c)
    b0 = moved(a0, across)
    a1, a3, a2 = [moved(a0, lambda x, y, z, c: (x - dx, y, z, c)) for dx in (1, 3, 2)]
    b1, b3 = [moved(b0, lambda x, y, z, c: (x - dx, y, z, c)) for dx in (1, 3)]
    b2 = moved(a2, across)
    return [a0, b0, a1, b1, a2, b2, a3, b3]


NT = (((1,), (1,)), ((), ()))


def kernel(counts, stored, emit, last, pos_ref, *refs):
    blocks = len(counts)
    x_refs, refs = refs[:2], refs[2:]
    w_refs = []
    for count in counts:
        w_refs.append(refs[:count])
        refs = refs[count:]
    total_blocks = 0 if emit else blocks + stored
    t_refs, refs = refs[: 8 * total_blocks], refs[8 * total_blocks :]
    s_refs, refs = refs[:stored], refs[stored:]
    o_ref, wbuf, tile, total = refs[-4:]
    acc_ref = refs[0] if len(refs) > 4 else None
    step = pl.program_id(0)

    @pl.when(step == 0)
    def _():
        row = 0
        for pieces in w_refs:
            for w_ref in pieces:
                wbuf[row : row + w_ref.shape[0]] = w_ref[...]
                row += w_ref.shape[0]
        if not emit:
            total[...] = jnp.zeros_like(total) if acc_ref is None else acc_ref[...]

    for h in range(2):
        rows = x_refs[h][...].reshape(DT * 32, -1)
        product = lax.dot_general(rows, wbuf[...], NT, preferred_element_type=jnp.float32)
        for lane in range(2 * blocks):
            tile[h, lane] = product[:, 128 * lane : 128 * (lane + 1)]

    def regrouped(n, q, h, a):
        lane, at = 2 * n + a // 2, (a % 2) * 64
        parts = [
            tile[h, lane, pl.ds(4 * q + d, 32, stride=DT), :][:, at : at + 64].astype(jnp.bfloat16)
            for d in range(4)
        ]
        return jnp.concatenate(parts, axis=1)

    for q in range(DT // 4):
        lefts = []
        for n in range(blocks):
            group = [regrouped(n, q, h, a) for h in range(2) for a in range(4)]
            lefts.append(jnp.concatenate(group, axis=0))
        if emit:
            for n in range(blocks):
                o_ref[n, q] = lefts[n]
            continue
        lefts += [s_ref[0, q] for s_ref in s_refs]
        for n in range(total_blocks):
            amp = jnp.concatenate(
                [t_refs[8 * n + r][0, :, 256 * q : 256 * (q + 1)] for r in range(8)], axis=0
            )
            total[...] += lax.dot_general(amp, lefts[n], NT, preferred_element_type=jnp.float32)

    if emit:
        return

    @pl.when(step == pl.num_programs(0) - 1)
    def _():
        if last:
            x, low, k = pos_ref[0], pos_ref[1], pos_ref[2]
            for dx in range(4):
                for dy in range(2):
                    to = lax.rem(x + dx, 4) * 2 + (low + dy) % 2
                    for e in range(2):
                        row = (dx * 2 + dy) * 16 + e * 8
                        o_ref[to, (k + e) % 2] = total[row : row + 8, :]
        else:
            o_ref[...] = total[...]


def contracted(pos, chol, window, amps, js, acc=None, stored=(), emit=False, last=False):
    blocks = len(js)
    n_d = chol[0].shape[1]
    full = lambda shape: pl.BlockSpec(shape, lambda i, pos: (0,) * len(shape))
    in_specs = [pl.BlockSpec((32, DT, 2048), lambda i, pos: (0, i, 0))] * 2
    operands = list(chol)
    for j in js:
        in_specs += [full(piece.shape) for piece in window[j]]
        operands += window[j]
    if not emit:
        for j in [*js, *(j for j, _, _ in stored)]:
            in_specs += [pl.BlockSpec((1, 16, DT * 64), lambda i, pos, j=j: (j, 0, i))] * 8
            operands += amps
    for _, left, n in stored:
        in_specs.append(pl.BlockSpec((1, DT // 4, 256, 256), lambda i, pos, n=n: (n, i, 0, 0)))
        operands.append(left)
    if acc is not None:
        in_specs.append(full((128, 256)))
        operands.append(acc)
    if emit:
        out = jax.ShapeDtypeStruct((blocks, n_d // 4, 256, 256), jnp.bfloat16)
        out_specs = pl.BlockSpec((blocks, DT // 4, 256, 256), lambda i, pos: (0, i, 0, 0))
    else:
        out = jax.ShapeDtypeStruct((8, 2, 8, 256) if last else (128, 256), jnp.float32)
        out_specs = full(out.shape)
    return pl.pallas_call(
        functools.partial(kernel, [len(window[j]) for j in js], len(stored), emit, last),
        grid_spec=pltpu.PrefetchScalarGridSpec(
            num_scalar_prefetch=1,
            grid=(n_d // DT,),
            in_specs=in_specs,
            out_specs=out_specs,
            scratch_shapes=[
                pltpu.VMEM((256 * blocks, 2048), jnp.bfloat16),
                pltpu.VMEM((2, 2 * blocks, DT * 32, 128), jnp.float32),
                pltpu.VMEM((128, 256), jnp.float32),
            ],
        ),
        out_shape=out,
        compiler_params=pltpu.CompilerParams(vmem_limit_bytes=VMEM_MIB * 1024 * 1024),
        cost_estimate=pl.CostEstimate(
            flops=blocks * 2 * 4096 * 256 * 2048, bytes_accessed=20 * 1024 * 1024, transcendentals=0
        ),
    )(pos, *operands)


def per_device(amplitudes, cholesky):
    x, y, z, k = position()
    pos = jnp.stack([x, y % 2, k]).astype(jnp.int32)
    swap = lambda x, y, z, c: (x, y, z, 1 - c)
    chol = (cholesky, moved(cholesky, swap))
    window = gathered_window(cholesky, x, y, k)
    amps = gathered_amplitudes(amplitudes, z, k)
    first = contracted(pos, chol, window, amps, (0,), emit=True)
    second = contracted(pos, chol, window, amps, (1, 3), emit=True)
    stored = ((0, first, 0), (1, second, 0), (3, second, 1))
    acc = contracted(pos, chol, window, amps, (2,), stored=stored, last=True)
    parts = acc.reshape(8, 16, 256)
    own = parts[:, :, :128] + moved(parts[:, :, 128:], swap)
    blocks = lax.all_to_all(own, "grp", 0, 0, tiled=True)
    result = jnp.sum(blocks, axis=0).reshape(16, 4, 32)
    result = lax.dynamic_slice_in_dim(jnp.concatenate([result, result], axis=1), (4 - x) % 4, 4, 1)
    return result.transpose(2, 1, 0)


def solution(mesh):
    in_specs = (P("pair", "grp", None), P("pair", "grp", None))
    out_specs = P("pair", None, "grp")
    return jax.shard_map(
        per_device, mesh=mesh, in_specs=in_specs, out_specs=out_specs, check_vma=False
    )
```

```python
import functools

import jax
import jax.numpy as jnp
from jax import lax
from jax.experimental import pallas as pl
from jax.experimental.pallas import tpu as pltpu
from jax.sharding import PartitionSpec as P


AXES = ("grp", "pair")
DT = 16
VMEM_MIB = 42


def linear(x, y, z, c):
    return ((y // 2) * 4 + z) * 16 + (x * 2 + y % 2) * 2 + c


def moved(value, where):
    pairs = []
    for x in range(4):
        for y in range(4):
            for z in range(4):
                for c in range(2):
                    to = where(x, y, z, c)
                    if to is not None:
                        pairs.append(
                            (linear(x, y, z, c), linear(to[0] % 4, to[1] % 4, to[2] % 4, to[3]))
                        )
    return lax.ppermute(value, AXES, pairs)


def position():
    g, p = lax.axis_index("grp"), lax.axis_index("pair")
    return p // 4, (g // 4) * 2 + (p // 2) % 2, g % 4, p % 2


def gathered_window(cholesky, x, y, k):
    at_root = lambda x, y, c: x == 0 and y % 2 == 0 and c == 0
    got = [
        moved(cholesky[dx], lambda x, y, z, c: (dx, y, z, y // 2) if at_root(x, y, c) else None)
        for dx in (1, 3, 2)
    ]
    got.append(
        moved(cholesky[0], lambda x, y, z, c: (0, y, z, 1) if at_root(x, y, c) and y == 2 else None)
    )
    own = jnp.where((x == 0) & (y == 0) & (k == 0), cholesky[0], jnp.zeros_like(cholesky[0]))
    piece = own + got[0] + got[1] + got[2] + got[3]
    spread = [
        moved(piece, lambda x, y, z, c: (x, y + dy, z, c) if y == 2 * c else None)
        for dy in (1, 3, 2)
    ]
    piece = piece + spread[0] + spread[1] + spread[2]
    others = [moved(piece, lambda x, y, z, c: (x - dx, y, z, c)) for dx in (1, 3, 2)]
    early = [moved(piece, lambda x, y, z, c: (x, y, z - j, c)) for j in (1, 3, 2)]
    half = others[2].shape[0] // 2
    upper = jnp.concatenate([others[0], others[2][:half]])
    lower = jnp.concatenate([others[2][half:], others[1]])
    rise = lambda x, y, z, c: (x, y, z + 1, c)
    fall = lambda x, y, z, c: (x, y, z - 1, c)
    up, down = moved(upper, rise), moved(lower, fall)
    up_more, down_more = moved(lower, rise), moved(upper, fall)
    up_far, down_far = moved(up, rise), moved(down, fall)
    return [
        [piece, upper, lower],
        [early[0], down_more, down],
        [early[2], up_far, down_far],
        [early[1], up, up_more],
    ]


def gathered_amplitudes(amplitudes, z, k):
    n_ij, n_d = amplitudes.shape[:2]
    parts = amplitudes.reshape(n_ij, n_d, 2, 4, 64).transpose(2, 3, 0, 1, 4).reshape(2, 4, n_ij, n_d * 64)
    twice = jnp.concatenate([parts, parts], axis=1)
    turned = lax.dynamic_slice_in_dim(twice, z, 4, 1)
    mine = lax.dynamic_index_in_dim(turned, k, 0, keepdims=False)
    other = lax.dynamic_index_in_dim(turned, 1 - k, 0, keepdims=False)
    came = moved(other, lambda x, y, z, c: (x, y, z, 1 - c))
    a0 = jnp.concatenate([mine, came], axis=1)
    across = lambda x, y, z, c: (x, y ^ 1, z, c)
    b0 = moved(a0, across)
    a1, a3, a2 = [moved(a0, lambda x, y, z, c: (x - dx, y, z, c)) for dx in (1, 3, 2)]
    b1, b3 = [moved(b0, lambda x, y, z, c: (x - dx, y, z, c)) for dx in (1, 3)]
    b2 = moved(a2, across)
    return [a0, b0, a1, b1, a2, b2, a3, b3]


NT = (((1,), (1,)), ((), ()))


def kernel(counts, stored, emit, last, pos_ref, *refs):
    blocks = len(counts)
    x_refs, refs = refs[:2], refs[2:]
    w_refs = []
    for count in counts:
        w_refs.append(refs[:count])
        refs = refs[count:]
    total_blocks = 0 if emit else blocks + stored
    t_refs, refs = refs[: 8 * total_blocks], refs[8 * total_blocks :]
    s_refs, refs = refs[:stored], refs[stored:]
    o_ref, wbuf, tile, total = refs[-4:]
    acc_ref = refs[0] if len(refs) > 4 else None
    step = pl.program_id(0)

    @pl.when(step == 0)
    def _():
        row = 0
        for pieces in w_refs:
            for w_ref in pieces:
                wbuf[row : row + w_ref.shape[0]] = w_ref[...]
                row += w_ref.shape[0]
        if not emit:
            total[...] = jnp.zeros_like(total) if acc_ref is None else acc_ref[...]

    for h in range(2):
        rows = x_refs[h][...].reshape(DT * 32, -1)
        product = lax.dot_general(rows, wbuf[...], NT, preferred_element_type=jnp.float32)
        for lane in range(2 * blocks):
            tile[h, lane] = product[:, 128 * lane : 128 * (lane + 1)]

    def regrouped(n, h, a):
        lane, at = 2 * n + a // 2, (a % 2) * 64
        parts = [
            tile[h, lane, pl.ds(d, 32, stride=DT), :][:, at : at + 64].astype(jnp.bfloat16)
            for d in range(DT)
        ]
        return jnp.concatenate(parts, axis=1)

    lefts = []
    for n in range(blocks):
        group = [regrouped(n, h, a) for h in range(2) for a in range(4)]
        lefts.append(jnp.concatenate(group, axis=0))
    if emit:
        for n in range(blocks):
            o_ref[n] = lefts[n]
    else:
        lefts = [s_ref[0] for s_ref in s_refs] + lefts
        partial = None
        for n in range(total_blocks):
            amp = jnp.concatenate([t_refs[8 * n + r][0] for r in range(8)], axis=0)
            term = lax.dot_general(amp, lefts[n], NT, preferred_element_type=jnp.float32)
            partial = term if partial is None else partial + term
        total[...] += partial

    if emit:
        return

    @pl.when(step == pl.num_programs(0) - 1)
    def _():
        if last:
            x, low, k, high, z = [pos_ref[i] for i in range(5)]
            for dx in range(4):
                for dy in range(2):
                    to = lax.rem(x + dx, 4) * 2 + (low + dy) % 2
                    to = lax.rem(to // 4 + high, 2) * 4 + lax.rem(to % 4 - z + 4, 4)
                    for e in range(2):
                        row = (dx * 2 + dy) * 16 + e * 8
                        o_ref[to, (k + e) % 2] = total[row : row + 8, :]
        else:
            o_ref[...] = total[...]


def contracted(pos, chol, window, amps, js, acc=None, stored=(), emit=False, last=False):
    blocks = len(js)
    n_d = chol[0].shape[1]
    full = lambda shape: pl.BlockSpec(shape, lambda i, pos: (0,) * len(shape))
    in_specs = [pl.BlockSpec((32, DT, 2048), lambda i, pos: (0, i, 0))] * 2
    operands = list(chol)
    for j in js:
        in_specs += [full(piece.shape) for piece in window[j]]
        operands += window[j]
    if not emit:
        for j in [*(j for j, _, _ in stored), *js]:
            in_specs += [pl.BlockSpec((1, 16, DT * 64), lambda i, pos, j=j: (j, 0, i))] * 8
            operands += amps
    for _, left, n in stored:
        in_specs.append(pl.BlockSpec((1, 256, DT * 64), lambda i, pos, n=n: (n, 0, i)))
        operands.append(left)
    if acc is not None:
        in_specs.append(full((128, 256)))
        operands.append(acc)
    if emit:
        out = jax.ShapeDtypeStruct((blocks, 256, n_d * 64), jnp.bfloat16)
        out_specs = pl.BlockSpec((blocks, 256, DT * 64), lambda i, pos: (0, 0, i))
    else:
        out = jax.ShapeDtypeStruct((8, 2, 8, 256) if last else (128, 256), jnp.float32)
        out_specs = full(out.shape)
    return pl.pallas_call(
        functools.partial(kernel, [len(window[j]) for j in js], len(stored), emit, last),
        grid_spec=pltpu.PrefetchScalarGridSpec(
            num_scalar_prefetch=1,
            grid=(n_d // DT,),
            in_specs=in_specs,
            out_specs=out_specs,
            scratch_shapes=[
                pltpu.VMEM((256 * blocks, 2048), jnp.bfloat16),
                pltpu.VMEM((2, 2 * blocks, DT * 32, 128), jnp.float32),
                pltpu.VMEM((128, 256), jnp.float32),
            ],
        ),
        out_shape=out,
        compiler_params=pltpu.CompilerParams(vmem_limit_bytes=VMEM_MIB * 1024 * 1024),
        cost_estimate=pl.CostEstimate(
            flops=blocks * 2 * 4096 * 256 * 2048, bytes_accessed=20 * 1024 * 1024, transcendentals=0
        ),
    )(pos, *operands)


def per_device(amplitudes, cholesky):
    x, y, z, k = position()
    pos = jnp.stack([x, y % 2, k, y // 2, z]).astype(jnp.int32)
    swap = lambda x, y, z, c: (x, y, z, 1 - c)
    chol = (cholesky, moved(cholesky, swap))
    window = gathered_window(cholesky, x, y, k)
    amps = gathered_amplitudes(amplitudes, z, k)
    first = contracted(pos, chol, window, amps, (0,), emit=True)
    second = contracted(pos, chol, window, amps, (1, 3), emit=True)
    stored = ((0, first, 0), (1, second, 0), (3, second, 1))
    acc = contracted(pos, chol, window, amps, (2,), stored=stored, last=True)
    parts = acc.reshape(8, 16, 256)
    own = parts[:, :, :128] + moved(parts[:, :, 128:], swap)
    half = own[:4] + moved(own[4:], lambda x, y, z, c: (x, y + 2, z, c))
    result = half[0]
    for j in (2, 1, 3):
        result = result + moved(half[j], lambda x, y, z, c: (x, y, z + j, c))
    result = result.reshape(16, 4, 32)
    result = lax.dynamic_slice_in_dim(jnp.concatenate([result, result], axis=1), (4 - x) % 4, 4, 1)
    return result.transpose(2, 1, 0)


def solution(mesh):
    in_specs = (P("pair", "grp", None), P("pair", "grp", None))
    out_specs = P("pair", None, "grp")
    return jax.shard_map(
        per_device, mesh=mesh, in_specs=in_specs, out_specs=out_specs, check_vma=False
    )
```

```python
import functools

import jax
import jax.numpy as jnp
from jax import lax
from jax.experimental import pallas as pl
from jax.experimental.pallas import tpu as pltpu
from jax.sharding import PartitionSpec as P


AXES = ("grp", "pair")
DT = 16
VMEM_MIB = 42
VMEM_FIRST = 50


def linear(x, y, z, c):
    return ((y // 2) * 4 + z) * 16 + (x * 2 + y % 2) * 2 + c


def moved(value, where):
    pairs = []
    for x in range(4):
        for y in range(4):
            for z in range(4):
                for c in range(2):
                    to = where(x, y, z, c)
                    if to is not None:
                        pairs.append(
                            (linear(x, y, z, c), linear(to[0] % 4, to[1] % 4, to[2] % 4, to[3]))
                        )
    return lax.ppermute(value, AXES, pairs)


def position():
    g, p = lax.axis_index("grp"), lax.axis_index("pair")
    return p // 4, (g // 4) * 2 + (p // 2) % 2, g % 4, p % 2


def gathered_window(cholesky, amplitudes, x, y, k):
    at_root = lambda x, y, c: x == 0 and y % 2 == 0 and c == 0
    got = [
        moved(cholesky[dx], lambda x, y, z, c: (dx, y, z, y // 2) if at_root(x, y, c) else None)
        for dx in (1, 3, 2)
    ]
    got.append(
        moved(cholesky[0], lambda x, y, z, c: (0, y, z, 1) if at_root(x, y, c) and y == 2 else None)
    )
    own = jnp.where((x == 0) & (y == 0) & (k == 0), cholesky[0], jnp.zeros_like(cholesky[0]))
    piece = own + got[0] + got[1] + got[2] + got[3]
    piece, amplitudes = lax.optimization_barrier((piece, amplitudes))
    spread = [
        moved(piece, lambda x, y, z, c: (x, y + dy, z, c) if y == 2 * c else None)
        for dy in (1, 3, 2)
    ]
    piece = piece + spread[0] + spread[1] + spread[2]
    others = [moved(piece, lambda x, y, z, c: (x - dx, y, z, c)) for dx in (1, 3, 2)]
    early = [moved(piece, lambda x, y, z, c: (x, y, z - j, c)) for j in (1, 3, 2)]
    half = others[2].shape[0] // 2
    upper = jnp.concatenate([others[0], others[2][:half]])
    lower = jnp.concatenate([others[2][half:], others[1]])
    rise = lambda x, y, z, c: (x, y, z + 1, c)
    fall = lambda x, y, z, c: (x, y, z - 1, c)
    up, down = moved(upper, rise), moved(lower, fall)
    up_more, down_more = moved(lower, rise), moved(upper, fall)
    up_far, down_far = moved(up, rise), moved(down, fall)
    window = [
        [piece, upper, lower],
        [early[0], down_more, down],
        [early[2], up_far, down_far],
        [early[1], up, up_more],
    ]
    return window, amplitudes


def relaid(pos, amplitudes):
    n_ij, n_d, n_c = amplitudes.shape

    def body(pos_ref, x_ref, o_ref, wide):
        k, z = pos_ref[2], pos_ref[4]
        for lane in range(n_c // 128):
            wide[lane] = x_ref[:, :, 128 * lane : 128 * (lane + 1)].astype(jnp.float32).reshape(-1, 128)
        for lane in range(n_c // 128):
            half = lax.rem(lane // 2 + k, 2)
            first = lax.rem(2 * (lane % 2) - z + 4, 4)
            second = lax.rem(2 * (lane % 2) + 1 - z + 4, 4)
            for d in range(0, n_d, 2):
                even = wide[lane, pl.ds(d, n_ij, stride=n_d), :]
                odd = wide[lane, pl.ds(d + 1, n_ij, stride=n_d), :]
                left = jnp.concatenate([even[:, :64], odd[:, :64]], axis=1).astype(jnp.bfloat16)
                right = jnp.concatenate([even[:, 64:], odd[:, 64:]], axis=1).astype(jnp.bfloat16)
                o_ref[half, first, :, 64 * d : 64 * d + 128] = left
                o_ref[half, second, :, 64 * d : 64 * d + 128] = right

    out = (2, 4, n_ij, n_d * 64)
    return pl.pallas_call(
        body,
        grid_spec=pltpu.PrefetchScalarGridSpec(
            num_scalar_prefetch=1,
            grid=(1,),
            in_specs=[pl.BlockSpec(amplitudes.shape, lambda i, pos: (0, 0, 0))],
            out_specs=pl.BlockSpec(out, lambda i, pos: (0, 0, 0, 0)),
            scratch_shapes=[pltpu.VMEM((n_c // 128, n_ij * n_d, 128), jnp.float32)],
        ),
        out_shape=jax.ShapeDtypeStruct(out, jnp.bfloat16),
        compiler_params=pltpu.CompilerParams(vmem_limit_bytes=8 * 1024 * 1024),
        cost_estimate=pl.CostEstimate(flops=1000000, bytes_accessed=1024 * 1024, transcendentals=0),
    )(pos, amplitudes)


def gathered_amplitudes(pos, amplitudes):
    mine, other = relaid(pos, amplitudes)
    came = moved(other, lambda x, y, z, c: (x, y, z, 1 - c))
    a0 = jnp.concatenate([mine, came], axis=1)
    across = lambda x, y, z, c: (x, y ^ 1, z, c)
    b0 = moved(a0, across)
    a1, a3, a2 = [moved(a0, lambda x, y, z, c: (x - dx, y, z, c)) for dx in (1, 3, 2)]
    b1, b3 = [moved(b0, lambda x, y, z, c: (x - dx, y, z, c)) for dx in (1, 3)]
    b2 = moved(a2, across)
    return [a0, b0, a1, b1, a2, b2, a3, b3]


NT = (((1,), (1,)), ((), ()))


def kernel(counts, stored, emit, last, pos_ref, *refs):
    blocks = len(counts)
    x_refs, refs = refs[:2], refs[2:]
    w_refs = []
    for count in counts:
        w_refs.append(refs[:count])
        refs = refs[count:]
    total_blocks = 0 if emit else blocks + stored
    t_refs, refs = refs[: 8 * total_blocks], refs[8 * total_blocks :]
    s_refs, refs = refs[:stored], refs[stored:]
    o_ref, wbuf, tile, total = refs[-4:]
    acc_ref = refs[0] if len(refs) > 4 else None
    step = pl.program_id(0)

    @pl.when(step == 0)
    def _():
        row = 0
        for pieces in w_refs:
            for w_ref in pieces:
                wbuf[row : row + w_ref.shape[0]] = w_ref[...]
                row += w_ref.shape[0]
        if not emit:
            total[...] = jnp.zeros_like(total) if acc_ref is None else acc_ref[...]

    for h in range(2):
        rows = x_refs[h][...].reshape(DT * 32, -1)
        product = lax.dot_general(rows, wbuf[...], NT, preferred_element_type=jnp.float32)
        for lane in range(2 * blocks):
            tile[h, lane] = product[:, 128 * lane : 128 * (lane + 1)]

    def regrouped(n, h, a):
        lane, at = 2 * n + a // 2, (a % 2) * 64
        parts = [
            tile[h, lane, pl.ds(d, 32, stride=DT), :][:, at : at + 64].astype(jnp.bfloat16)
            for d in range(DT)
        ]
        return jnp.concatenate(parts, axis=1)

    lefts = []
    for n in range(blocks):
        group = [regrouped(n, h, a) for h in range(2) for a in range(4)]
        lefts.append(jnp.concatenate(group, axis=0))
    if emit:
        for n in range(blocks):
            o_ref[n] = lefts[n]
    else:
        lefts = [s_ref[0] for s_ref in s_refs] + lefts
        partial = None
        for n in range(total_blocks):
            amp = jnp.concatenate([t_refs[8 * n + r][0] for r in range(8)], axis=0)
            term = lax.dot_general(amp, lefts[n], NT, preferred_element_type=jnp.float32)
            partial = term if partial is None else partial + term
        total[...] += partial

    if emit:
        return

    @pl.when(step == pl.num_programs(0) - 1)
    def _():
        if last:
            x, low, k, high, z = [pos_ref[i] for i in range(5)]
            for dx in range(4):
                for dy in range(2):
                    to = lax.rem(x + dx, 4) * 2 + (low + dy) % 2
                    to = lax.rem(to // 4 + high, 2) * 4 + lax.rem(to % 4 - z + 4, 4)
                    for e in range(2):
                        row = (dx * 2 + dy) * 16 + e * 8
                        o_ref[to, (k + e) % 2] = total[row : row + 8, :]
        else:
            o_ref[...] = total[...]


def contracted(pos, chol, window, amps, js, acc=None, stored=(), emit=False, last=False):
    blocks = len(js)
    n_d = chol[0].shape[1]
    full = lambda shape: pl.BlockSpec(shape, lambda i, pos: (0,) * len(shape))
    in_specs = [pl.BlockSpec((32, DT, 2048), lambda i, pos: (0, i, 0))] * 2
    operands = list(chol)
    for j in js:
        in_specs += [full(piece.shape) for piece in window[j]]
        operands += window[j]
    if not emit:
        for j in [*(j for j, _, _ in stored), *js]:
            in_specs += [pl.BlockSpec((1, 16, DT * 64), lambda i, pos, j=j: (j, 0, i))] * 8
            operands += amps
    for _, left, n in stored:
        in_specs.append(pl.BlockSpec((1, 256, DT * 64), lambda i, pos, n=n: (n, 0, i)))
        operands.append(left)
    if acc is not None:
        in_specs.append(full((128, 256)))
        operands.append(acc)
    if emit:
        out = jax.ShapeDtypeStruct((blocks, 256, n_d * 64), jnp.bfloat16)
        out_specs = pl.BlockSpec((blocks, 256, DT * 64), lambda i, pos: (0, 0, i))
    else:
        out = jax.ShapeDtypeStruct((8, 2, 8, 256) if last else (128, 256), jnp.float32)
        out_specs = full(out.shape)
    return pl.pallas_call(
        functools.partial(kernel, [len(window[j]) for j in js], len(stored), emit, last),
        grid_spec=pltpu.PrefetchScalarGridSpec(
            num_scalar_prefetch=1,
            grid=(n_d // DT,),
            in_specs=in_specs,
            out_specs=out_specs,
            scratch_shapes=[
                pltpu.VMEM((256 * blocks, 2048), jnp.bfloat16),
                pltpu.VMEM((2, 2 * blocks, DT * 32, 128), jnp.float32),
                pltpu.VMEM((128, 256), jnp.float32),
            ],
        ),
        out_shape=out,
        compiler_params=pltpu.CompilerParams(vmem_limit_bytes=(VMEM_FIRST if emit and blocks == 1 else VMEM_MIB) * 1024 * 1024),
        cost_estimate=pl.CostEstimate(
            flops=blocks * 2 * 4096 * 256 * 2048, bytes_accessed=20 * 1024 * 1024, transcendentals=0
        ),
    )(pos, *operands)


def per_device(amplitudes, cholesky):
    x, y, z, k = position()
    pos = jnp.stack([x, y % 2, k, y // 2, z]).astype(jnp.int32)
    swap = lambda x, y, z, c: (x, y, z, 1 - c)
    chol = (cholesky, moved(cholesky, swap))
    window, amplitudes = gathered_window(cholesky, amplitudes, x, y, k)
    amps = gathered_amplitudes(pos, amplitudes)
    first = contracted(pos, chol, window, amps, (0,), emit=True)
    second = contracted(pos, chol, window, amps, (1, 3), emit=True)
    stored = ((0, first, 0), (1, second, 0), (3, second, 1))
    acc = contracted(pos, chol, window, amps, (2,), stored=stored, last=True)
    parts = acc.reshape(8, 16, 256)
    own = parts[:, :, :128] + moved(parts[:, :, 128:], swap)
    half = own[:4] + moved(own[4:], lambda x, y, z, c: (x, y + 2, z, c))
    result = half[0]
    for j in (2, 1, 3):
        result = result + moved(half[j], lambda x, y, z, c: (x, y, z + j, c))
    result = result.reshape(16, 4, 32)
    result = lax.dynamic_slice_in_dim(jnp.concatenate([result, result], axis=1), (4 - x) % 4, 4, 1)
    return result.transpose(2, 1, 0)


def solution(mesh):
    in_specs = (P("pair", "grp", None), P("pair", "grp", None))
    out_specs = P("pair", None, "grp")
    return jax.shard_map(
        per_device, mesh=mesh, in_specs=in_specs, out_specs=out_specs, check_vma=False
    )
```
